8 devices in a mesh: dp: 1 (over z), ep: 8 (over y, x, core).
Axes of the slice: x: 2, y: 2, z: 1, core: 2. Of those that a mesh axis runs over, the one named last changes fastest.
Arguments:
- tokens: bfloat16 [32768, 1536], P(('dp', 'ep'))
- routes: int32 [32768, 8], P(('dp', 'ep'))
- w_router: bfloat16 [1536, 40], replicated
- w_one: bfloat16 [40, 1536, 512], P('ep')
- w_three: bfloat16 [40, 1536, 512], P('ep')
- w_two: bfloat16 [40, 512, 1536], P('ep')
Outputs:
- output: bfloat16 [32768, 1536], P(('dp', 'ep'))
All inputs are finite; a program needn't handle non-finite values.
Results may differ from the reference program's by a relative error of at most 0.00818649.
Values are sent between devices in bfloat16 or wider.
A program may use at most 1 GiB of HBM per device.

```python
import jax
import jax.numpy as jnp
from jax import lax

GROUP_SIZE = 8
DEV_TOKENS = 4096
D_MODEL = 1536
D_EXPERT = 512
NUM_EXPERTS = 40
TOP_K = 8
CAPACITY = 1232


def draw_routes(route_key):
    perm_key, row_key, slot_key = jax.random.split(route_key, 3)
    num_pairs = DEV_TOKENS * TOP_K
    hot_count = NUM_EXPERTS // 8
    rest_pairs = num_pairs - hot_count * CAPACITY
    base_count = rest_pairs // (NUM_EXPERTS - hot_count)
    extra_count = rest_pairs % (NUM_EXPERTS - hot_count)
    rank_ids = jnp.arange(NUM_EXPERTS, dtype=jnp.int32)
    counts = jnp.where(rank_ids < hot_count, CAPACITY, base_count + (rank_ids - hot_count < extra_count).astype(jnp.int32))
    count_ends = jnp.cumsum(counts)
    pair_rank = jnp.searchsorted(count_ends, jnp.arange(num_pairs, dtype=jnp.int32), side='right')
    expert_of_rank = jax.random.permutation(perm_key, NUM_EXPERTS)
    layout = expert_of_rank[pair_rank].reshape(TOP_K, DEV_TOKENS).T

    def device_routes(perm_rows, perm_slots):
        row_order = jax.random.permutation(perm_rows, DEV_TOKENS)
        scores = jax.random.randint(perm_slots, (DEV_TOKENS, TOP_K), 0, 1 << 20) * TOP_K + jnp.arange(TOP_K)
        slot_order = jnp.argsort(scores, axis=1)
        return jnp.take_along_axis(layout[row_order], slot_order, axis=1)

    per_device = jax.vmap(device_routes)(jax.random.split(row_key, GROUP_SIZE), jax.random.split(slot_key, GROUP_SIZE))
    return per_device.reshape(GROUP_SIZE * DEV_TOKENS, TOP_K).astype(jnp.int32)


def setup_inputs(seed: int = 0, part: int = 0) -> dict:
    part_key = jax.random.fold_in(jax.random.key(seed), part)
    token_key, route_key = jax.random.split(part_key)
    shared = jax.random.split(jax.random.key(seed + 1), 4)
    tokens = jax.random.normal(token_key, (GROUP_SIZE * DEV_TOKENS, D_MODEL), jnp.float32)
    w_router = jax.random.normal(shared[0], (D_MODEL, NUM_EXPERTS), jnp.float32) * (1.5 * D_MODEL ** -0.5)
    w_one = jax.random.normal(shared[1], (NUM_EXPERTS, D_MODEL, D_EXPERT), jnp.float32) * D_MODEL ** -0.5
    w_three = jax.random.normal(shared[2], (NUM_EXPERTS, D_MODEL, D_EXPERT), jnp.float32) * D_MODEL ** -0.5
    w_two = jax.random.normal(shared[3], (NUM_EXPERTS, D_EXPERT, D_MODEL), jnp.float32) * D_EXPERT ** -0.5
    return {'tokens': tokens.astype(jnp.bfloat16), 'routes': draw_routes(route_key), 'w_router': w_router.astype(jnp.bfloat16), 'w_one': w_one.astype(jnp.bfloat16), 'w_three': w_three.astype(jnp.bfloat16), 'w_two': w_two.astype(jnp.bfloat16)}


def expert_rows(rows, w_gate, w_up, w_down):
    gate_pre = jnp.dot(rows, w_gate, preferred_element_type=jnp.float32)
    up_pre = jnp.dot(rows, w_up, preferred_element_type=jnp.float32)
    hidden = (jax.nn.silu(gate_pre) * up_pre).astype(jnp.bfloat16)
    return jnp.dot(hidden, w_down, preferred_element_type=jnp.float32).astype(jnp.bfloat16)


def reference(tokens, routes, w_router, w_one, w_three, w_two):
    logits = jnp.dot(tokens, w_router, preferred_element_type=jnp.float32)
    gate_vals = jax.nn.softmax(jnp.take_along_axis(logits, routes, axis=1), axis=-1)
    flat_gates = gate_vals.reshape(-1)
    flat_routes = routes.reshape(-1)
    num_pairs = flat_routes.shape[0]
    sort_order = jnp.argsort(flat_routes, stable=True)
    counts = jax.ops.segment_sum(jnp.ones_like(flat_routes), flat_routes, num_segments=NUM_EXPERTS)
    starts = jnp.cumsum(counts) - counts
    slot_ids = jnp.arange(GROUP_SIZE * CAPACITY, dtype=jnp.int32)

    def one_expert(y_sum, step_in):
        w_gate, w_up, w_down, exp_start, exp_count = step_in
        pair_at = sort_order[jnp.minimum(exp_start + slot_ids, num_pairs - 1)]
        token_at = pair_at // TOP_K
        weight = jnp.where(slot_ids < exp_count, flat_gates[pair_at], 0.0)
        out_rows = expert_rows(tokens[token_at], w_gate, w_up, w_down)
        return y_sum.at[token_at].add(weight[:, None] * out_rows.astype(jnp.float32)), None

    y_sum = lax.scan(one_expert, jnp.zeros(tokens.shape, jnp.float32), (w_one, w_three, w_two, starts, counts))[0]
    return y_sum.astype(jnp.bfloat16)
```

```python
import functools

import jax
import jax.numpy as jnp
from jax import lax
from jax.experimental import pallas as pl
from jax.experimental.pallas import tpu as pltpu
from jax.sharding import PartitionSpec as P

LANES = 128
SUBLANES = 8
TILE = 256
UNROLL = 8


def route_lists(tokens, routes, w_router):
    num_tokens, top_k = routes.shape
    num_experts = w_router.shape[1]
    chunks = tokens.shape[1] // LANES
    logits = jnp.dot(tokens, w_router, preferred_element_type=jnp.float32).T
    slots = routes.T
    experts = jnp.arange(num_experts, dtype=jnp.int32)
    hit = slots[:, None, :] == experts[None, :, None]
    picked = jnp.sum(jnp.where(hit, logits[None], 0.0), axis=1)
    gates = jax.nn.softmax(picked, axis=0)
    counts = jnp.sum(hit, axis=(0, 2), dtype=jnp.int32)
    starts = jnp.cumsum(counts) - counts
    keys = slots * num_tokens + jnp.arange(num_tokens, dtype=jnp.int32)[None, :]
    keys, gates = lax.sort((keys.reshape(-1), gates.reshape(-1)), num_keys=1, is_stable=False)
    token_at = keys % num_tokens
    address = (token_at // SUBLANES) * (SUBLANES * chunks) + token_at % SUBLANES
    return jnp.pad(address, (0, TILE)), jnp.pad(gates, (0, TILE)), starts, counts


def to_tiles(rows):
    num_rows, width = rows.shape
    tiled = rows.reshape(num_rows // SUBLANES, SUBLANES, width // LANES, LANES)
    return tiled.transpose(0, 2, 1, 3).reshape(num_rows * (width // LANES), LANES)


def stage_kernel(first, last, num_stage, d_model, starts, counts, address, gates, x_hbm, *refs):
    if first:
        w_one, w_three, w_two, out, x_v, y_v, one_v, three_v, two_v, rows_v, outs_v, cast_v, w_sem, io_sem = refs
        y_hbm = None
    else:
        y_hbm, w_one, w_three, w_two, out, x_v, y_v, one_v, three_v, two_v, rows_v, outs_v, cast_v, w_sem, io_sem = refs
    chunks = d_model // LANES

    def weight_copies(e):
        slot = lax.rem(e, 2)
        return [
            pltpu.make_async_copy(src.at[e], dst.at[slot], w_sem.at[slot, i])
            for i, (src, dst) in enumerate(((w_one, one_v), (w_three, three_v), (w_two, two_v)))
        ]

    x_copy = pltpu.make_async_copy(x_hbm, x_v, io_sem.at[0])
    x_copy.start()
    for copy in weight_copies(0):
        copy.start()
    if first:
        def clear(i, _):
            y_v[pl.ds(pl.multiple_of(i * 256, 256), 256), :] = jnp.zeros((256, LANES), jnp.float32)
            return 0
        lax.fori_loop(0, y_v.shape[0] // 256, clear, 0)
    else:
        y_copy = pltpu.make_async_copy(y_hbm, y_v, io_sem.at[1])
        y_copy.start()
        y_copy.wait()
    x_copy.wait()

    def row_slice(base):
        return pl.ds(base, chunks, stride=SUBLANES)

    def expert(e, _):
        slot = lax.rem(e, 2)

        @pl.when(e + 1 < num_stage)
        def _():
            for copy in weight_copies(e + 1):
                copy.start()

        for copy in weight_copies(e):
            copy.wait()
        begin = starts[e]
        count = counts[e]

        def tile(t, _):
            tile_begin = begin + t * TILE
            live = jnp.minimum(count - t * TILE, TILE)

            def gather(g, _):
                at = tile_begin + g * SUBLANES
                rows = [x_v[row_slice(address[at + u]), :] for u in range(SUBLANES)]
                for u in range(SUBLANES):
                    rows_v[row_slice(g * (SUBLANES * chunks) + u), :] = rows[u]
                return 0

            lax.fori_loop(0, TILE // SUBLANES, gather, 0)
            tiled = rows_v[...].reshape(TILE // SUBLANES, chunks, SUBLANES, LANES)
            lhs = jnp.concatenate([tiled[:, c].reshape(TILE, LANES).astype(jnp.bfloat16) for c in range(chunks)], axis=1)
            gate_pre = jnp.dot(lhs, one_v[slot], preferred_element_type=jnp.float32)
            up_pre = jnp.dot(lhs, three_v[slot], preferred_element_type=jnp.float32)
            hidden = (jax.nn.silu(gate_pre) * up_pre).astype(jnp.bfloat16)
            down = jnp.dot(hidden, two_v[slot], preferred_element_type=jnp.float32)
            down = down.astype(jnp.bfloat16).astype(jnp.float32)
            parts = [down[:, c * LANES:(c + 1) * LANES].reshape(TILE // SUBLANES, 1, SUBLANES, LANES) for c in range(chunks)]
            outs_v[...] = jnp.concatenate(parts, axis=1).reshape(TILE * chunks, LANES)

            def add_rows(first_row, size, local):
                at = [tile_begin + first_row + u for u in range(size)]
                where = [address[a] for a in at]
                sums = [y_v[row_slice(w), :] for w in where]
                terms = [outs_v[row_slice(local + u), :] * gates[a] for u, a in enumerate(at)]
                for u in range(size):
                    y_v[row_slice(where[u]), :] = sums[u] + terms[u]

            def scatter(g, _):
                add_rows(g * SUBLANES, SUBLANES, g * (SUBLANES * chunks))
                return 0

            full = live // SUBLANES
            lax.fori_loop(0, full, scatter, 0)

            def scatter_one(r, _):
                add_rows(full * SUBLANES + r, 1, full * (SUBLANES * chunks) + r)
                return 0

            lax.fori_loop(0, live - full * SUBLANES, scatter_one, 0)
            return 0

        lax.fori_loop(0, (count + TILE - 1) // TILE, tile, 0)
        return 0

    lax.fori_loop(0, num_stage, expert, 0)

    if last:
        block = cast_v.shape[1]
        steps = (y_v.shape[0] // chunks) // block

        def out_copy(i):
            return pltpu.make_async_copy(cast_v.at[lax.rem(i, 2)], out.at[pl.ds(pl.multiple_of(i * block, block), block)], io_sem.at[lax.rem(i, 2)])

        def finish(i, _):
            @pl.when(i >= 2)
            def _():
                out_copy(i - 2).wait()
            part = y_v[pl.ds(pl.multiple_of(i * (block * chunks), block * chunks), block * chunks), :].reshape(block // SUBLANES, chunks, SUBLANES, LANES)
            cast_v[lax.rem(i, 2)] = jnp.concatenate([part[:, c].reshape(block, LANES).astype(jnp.bfloat16) for c in range(chunks)], axis=1)
            out_copy(i).start()
            return 0

        lax.fori_loop(0, steps, finish, 0)
        out_copy(steps - 2).wait()
        out_copy(steps - 1).wait()
    else:
        out_copy = pltpu.make_async_copy(y_v, out, io_sem.at[0])
        out_copy.start()
        out_copy.wait()


def run_stage(x_tiles, y_tiles, starts, counts, address, gates, w_one, w_three, w_two, last):
    num_stage, d_model, d_expert = w_one.shape
    chunks = d_model // LANES
    num_rows = x_tiles.shape[0] // chunks
    first = y_tiles is None
    smem = pl.BlockSpec(memory_space=pltpu.SMEM)
    hbm = pl.BlockSpec(memory_space=pl.ANY)
    arrays = [x_tiles] + ([] if first else [y_tiles]) + [w_one, w_three, w_two]
    if last:
        out_shape = jax.ShapeDtypeStruct((num_rows, d_model), jnp.bfloat16)
    else:
        out_shape = jax.ShapeDtypeStruct(x_tiles.shape, jnp.float32)
    return pl.pallas_call(
        functools.partial(stage_kernel, first, last, num_stage, d_model),
        out_shape=out_shape,
        in_specs=[smem] * 4 + [hbm] * len(arrays),
        out_specs=hbm,
        scratch_shapes=[
            pltpu.VMEM(x_tiles.shape, jnp.float32),
            pltpu.VMEM(x_tiles.shape, jnp.float32),
            pltpu.VMEM((2, d_model, d_expert), jnp.bfloat16),
            pltpu.VMEM((2, d_model, d_expert), jnp.bfloat16),
            pltpu.VMEM((2, d_expert, d_model), jnp.bfloat16),
            pltpu.VMEM((TILE * chunks, LANES), jnp.float32),
            pltpu.VMEM((TILE * chunks, LANES), jnp.float32),
            pltpu.VMEM((2, 64, d_model), jnp.bfloat16),
            pltpu.SemaphoreType.DMA((2, 3)),
            pltpu.SemaphoreType.DMA((2,)),
        ],
        input_output_aliases={} if first or last else {5: 0},
        compiler_params=pltpu.CompilerParams(vmem_limit_bytes=67_043_328),
        cost_estimate=pl.CostEstimate(flops=num_stage * 820 * 6 * d_model * d_expert, bytes_accessed=num_stage * 6 * d_model * d_expert, transcendentals=0),
        name=f"experts_{num_stage}",
    )(starts, counts, address, gates, *arrays)


def solution(mesh):
    row_spec = P(("dp", "ep"), None)
    expert_spec = P("ep", None, None)

    def device_step(tokens, routes, w_router, w_one, w_three, w_two):
        address, gates, starts, counts = route_lists(tokens, routes, w_router)
        x_tiles = to_tiles(tokens.astype(jnp.float32))
        full = [lax.all_gather(w, "ep", axis=0, tiled=True) for w in (w_one, w_three, w_two)]
        return run_stage(x_tiles, None, starts, counts, address, gates, *full, last=True)

    return jax.shard_map(device_step, mesh=mesh, in_specs=(row_spec, row_spec, P(None, None), expert_spec, expert_spec, expert_spec), out_specs=row_spec, check_vma=False)
```

```python
import functools

import jax
import jax.numpy as jnp
from jax import lax
from jax.experimental import pallas as pl
from jax.experimental.pallas import tpu as pltpu
from jax.sharding import PartitionSpec as P


LANES = 128
SUBLANES = 8
TILE = 256
COST_FLOPS = 4_000_000_000


def route_lists(tokens, routes, w_router):
    num_tokens, _ = routes.shape
    num_experts = w_router.shape[1]
    chunks = tokens.shape[1] // LANES
    logits = jnp.dot(tokens, w_router, preferred_element_type=jnp.float32).T
    slots = routes.T
    experts = jnp.arange(num_experts, dtype=jnp.int32)
    hit = slots[:, None, :] == experts[None, :, None]
    picked = jnp.sum(jnp.where(hit, logits[None], 0.0), axis=1)
    gates = jax.nn.softmax(picked, axis=0)
    counts = jnp.sum(hit, axis=(0, 2), dtype=jnp.int32)
    starts = jnp.cumsum(counts) - counts
    keys = slots * num_tokens + jnp.arange(num_tokens, dtype=jnp.int32)[None, :]
    keys, gates = lax.sort((keys.reshape(-1), gates.reshape(-1)), num_keys=1, is_stable=False)
    token_at = keys % num_tokens
    address = (token_at // SUBLANES) * (SUBLANES * chunks) + token_at % SUBLANES
    return jnp.pad(address, (0, TILE)), jnp.pad(gates, (0, TILE)), starts, counts


def to_tiles(rows):
    num_rows, width = rows.shape
    tiled = rows.reshape(num_rows // SUBLANES, SUBLANES, width // LANES, LANES)
    return tiled.transpose(0, 2, 1, 3).reshape(num_rows * (width // LANES), LANES)


def pack_kernel(cuts, w_one, w_three, w_two, *refs):
    outs, (buffer, in_sem, out_sem) = refs[:len(cuts)], refs[len(cuts):]
    slots = sorted({s for s, _, _ in cuts})
    d_expert = w_one.shape[2]

    def loads(i, s):
        pairs = [(w_one.at[s], buffer.at[i, 0]), (w_three.at[s], buffer.at[i, 1])]
        for c in range(w_two.shape[2] // d_expert):
            pairs.append((w_two.at[s, :, pl.ds(c * d_expert, d_expert)], buffer.at[i, 2, pl.ds(c * d_expert, d_expert)]))
        return [pltpu.make_async_copy(a, b, in_sem.at[i, j]) for j, (a, b) in enumerate(pairs)]

    stores = [
        pltpu.make_async_copy(buffer.at[slots.index(s), :, pl.ds(row, size)], outs[k], out_sem.at[k])
        for k, (s, row, size) in enumerate(cuts)
    ]
    for i, s in enumerate(slots):
        for copy in loads(i, s):
            copy.start()
    for i, s in enumerate(slots):
        for copy in loads(i, s):
            copy.wait()
        for k, cut in enumerate(cuts):
            if cut[0] == s:
                stores[k].start()
    for copy in stores:
        copy.wait()


def pack(cuts, w_one, w_three, w_two):
    _, d_model, d_expert = w_one.shape
    num_slots = len({s for s, _, _ in cuts})
    return pl.pallas_call(
        functools.partial(pack_kernel, cuts),
        out_shape=[jax.ShapeDtypeStruct((3, size, d_expert), w_one.dtype) for _, _, size in cuts],
        in_specs=[pl.BlockSpec(memory_space=pl.ANY)] * 3,
        out_specs=[pl.BlockSpec(memory_space=pl.ANY)] * len(cuts),
        scratch_shapes=[
            pltpu.VMEM((num_slots, 3, d_model, d_expert), w_one.dtype),
            pltpu.SemaphoreType.DMA((num_slots, 2 + d_model // d_expert)),
            pltpu.SemaphoreType.DMA((len(cuts),)),
        ],
    )(w_one, w_three, w_two)


def stage_kernel(first, last, offset, plan, d_model, d_expert, starts, counts, address, gates, x_hbm, *refs):
    refs = list(refs)
    y_hbm = None if first else refs.pop(0)
    num_arrays = 1 + max(piece[0] for pieces in plan for piece in pieces)
    weights, refs = refs[:num_arrays], refs[num_arrays:]
    out, x_v, y_v, w_v, rows_v, outs_v, cast_v, w_sem, io_sem = refs
    chunks = d_model // LANES
    num_stage = len(plan)

    def start_weights(step):
        slot = lax.rem(step, 2)
        for i, pieces in enumerate(plan):
            @pl.when(step == i)
            def _(pieces=pieces):
                for array, source, target in pieces:
                    pltpu.make_async_copy(weights[array].at[source], w_v.at[(slot,) + target], w_sem.at[slot]).start()

    def wait_weights(step):
        slot = lax.rem(step, 2)
        pltpu.make_async_copy(w_v.at[slot], w_v.at[slot], w_sem.at[slot]).wait()

    x_copy = pltpu.make_async_copy(x_hbm, x_v, io_sem.at[0])
    x_copy.start()
    start_weights(0)
    if first:
        def clear(i, _):
            y_v[pl.ds(pl.multiple_of(i * 256, 256), 256), :] = jnp.zeros((256, LANES), jnp.float32)
            return 0

        lax.fori_loop(0, y_v.shape[0] // 256, clear, 0)
    else:
        y_copy = pltpu.make_async_copy(y_hbm, y_v, io_sem.at[1])
        y_copy.start()
        y_copy.wait()
    x_copy.wait()

    def row_slice(base):
        return pl.ds(base, chunks, stride=SUBLANES)

    def expert(e, _):
        slot = lax.rem(e, 2)
        start_weights(e + 1)
        wait_weights(e)
        begin = starts[offset + e]
        count = counts[offset + e]

        def tile(t, _):
            tile_begin = begin + t * TILE
            live = jnp.minimum(count - t * TILE, TILE)

            def gather(g, _):
                at = tile_begin + g * SUBLANES
                rows = [x_v[row_slice(address[at + u]), :] for u in range(SUBLANES)]
                for u in range(SUBLANES):
                    rows_v[row_slice(g * (SUBLANES * chunks) + u), :] = rows[u]
                return 0

            lax.fori_loop(0, TILE // SUBLANES, gather, 0)
            tiled = rows_v[...].reshape(TILE // SUBLANES, chunks, SUBLANES, LANES)
            lhs = jnp.concatenate([tiled[:, c].reshape(TILE, LANES).astype(jnp.bfloat16) for c in range(chunks)], axis=1)
            gate_pre = jnp.dot(lhs, w_v[slot, 0], preferred_element_type=jnp.float32)
            up_pre = jnp.dot(lhs, w_v[slot, 1], preferred_element_type=jnp.float32)
            hidden = (jax.nn.silu(gate_pre) * up_pre).astype(jnp.bfloat16)
            parts = []
            for c in range(d_model // d_expert):
                down = jnp.dot(hidden, w_v[slot, 2, c * d_expert:(c + 1) * d_expert], preferred_element_type=jnp.float32)
                down = down.astype(jnp.bfloat16).astype(jnp.float32)
                for k in range(d_expert // LANES):
                    parts.append(down[:, k * LANES:(k + 1) * LANES].reshape(TILE // SUBLANES, 1, SUBLANES, LANES))
            outs_v[...] = jnp.concatenate(parts, axis=1).reshape(TILE * chunks, LANES)

            def add_rows(first_row, size, local):
                at = [tile_begin + first_row + u for u in range(size)]
                where = [address[a] for a in at]
                sums = [y_v[row_slice(w), :] for w in where]
                terms = [outs_v[row_slice(local + u), :] * gates[a] for u, a in enumerate(at)]
                for u in range(size):
                    y_v[row_slice(where[u]), :] = sums[u] + terms[u]

            def scatter(g, _):
                add_rows(g * SUBLANES, SUBLANES, g * (SUBLANES * chunks))
                return 0

            full = live // SUBLANES
            lax.fori_loop(0, full, scatter, 0)

            def scatter_one(r, _):
                add_rows(full * SUBLANES + r, 1, full * (SUBLANES * chunks) + r)
                return 0

            lax.fori_loop(0, live - full * SUBLANES, scatter_one, 0)
            return 0

        lax.fori_loop(0, (count + TILE - 1) // TILE, tile, 0)
        return 0

    lax.fori_loop(0, num_stage, expert, 0)

    if last:
        block = cast_v.shape[1]
        steps = (y_v.shape[0] // chunks) // block

        def out_copy(i):
            return pltpu.make_async_copy(cast_v.at[lax.rem(i, 2)], out.at[pl.ds(pl.multiple_of(i * block, block), block)], io_sem.at[lax.rem(i, 2)])

        def finish(i, _):
            @pl.when(i >= 2)
            def _():
                out_copy(i - 2).wait()

            part = y_v[pl.ds(pl.multiple_of(i * (block * chunks), block * chunks), block * chunks), :].reshape(block // SUBLANES, chunks, SUBLANES, LANES)
            cast_v[lax.rem(i, 2)] = jnp.concatenate([part[:, c].reshape(block, LANES).astype(jnp.bfloat16) for c in range(chunks)], axis=1)
            out_copy(i).start()
            return 0

        lax.fori_loop(0, steps, finish, 0)
        out_copy(steps - 2).wait()
        out_copy(steps - 1).wait()
    else:
        out_copy = pltpu.make_async_copy(y_v, out, io_sem.at[0])
        out_copy.start()
        out_copy.wait()


def run_stage(x_tiles, y_tiles, starts, counts, address, gates, offset, entries, shape, last):
    arrays, plan = [], []
    for entry in entries:
        pieces = []
        for array, source, target in entry:
            at = next((i for i, known in enumerate(arrays) if known is array), None)
            if at is None:
                at = len(arrays)
                arrays.append(array)
            pieces.append((at, source, target))
        plan.append(tuple(pieces))
    d_model, d_expert = shape
    chunks = d_model // LANES
    num_rows = x_tiles.shape[0] // chunks
    first = y_tiles is None
    smem = pl.BlockSpec(memory_space=pltpu.SMEM)
    hbm = pl.BlockSpec(memory_space=pl.ANY)
    operands = [x_tiles] + ([] if first else [y_tiles]) + arrays
    if last:
        out_shape = jax.ShapeDtypeStruct((num_rows, d_model), jnp.bfloat16)
    else:
        out_shape = jax.ShapeDtypeStruct(x_tiles.shape, jnp.float32)
    return pl.pallas_call(
        functools.partial(stage_kernel, first, last, offset, tuple(plan), d_model, d_expert),
        out_shape=out_shape,
        in_specs=[smem] * 4 + [hbm] * len(operands),
        out_specs=hbm,
        scratch_shapes=[
            pltpu.VMEM(x_tiles.shape, jnp.float32),
            pltpu.VMEM(x_tiles.shape, jnp.float32),
            pltpu.VMEM((2, 3, d_model, d_expert), jnp.bfloat16),
            pltpu.VMEM((TILE * chunks, LANES), jnp.float32),
            pltpu.VMEM((TILE * chunks, LANES), jnp.float32),
            pltpu.VMEM((2, 64, d_model), jnp.bfloat16),
            pltpu.SemaphoreType.DMA((2,)),
            pltpu.SemaphoreType.DMA((2,)),
        ],
        input_output_aliases={} if first or last else {5: 0},
        compiler_params=pltpu.CompilerParams(vmem_limit_bytes=67_043_328),
        cost_estimate=pl.CostEstimate(flops=len(plan) * COST_FLOPS, bytes_accessed=len(plan) * 6 * d_model * d_expert, transcendentals=0),
    )(starts, counts, address, gates, *operands)


def solution(mesh):
    row_spec = P(("dp", "ep"), None)
    expert_spec = P("ep", None, None)
    size = mesh.shape["ep"]

    def hop(array, mask):
        return lax.ppermute(array, "ep", [(i, i ^ mask) for i in range(size)])

    def device_step(tokens, routes, w_router, *own):
        local, d_model, d_expert = own[0].shape
        half = d_model // 2
        blocks = d_model // d_expert
        here = {}

        def note(mask, w_one, w_three, w_two):
            for s in range(local):
                here[mask, s] = [(w_one, (s,), (0,)), (w_three, (s,), (1,))] + [
                    (w_two, (s, slice(None), pl.ds(c * d_expert, d_expert)), (2, pl.ds(c * d_expert, d_expert))) for c in range(blocks)
                ]

        note(0, *own)
        note(1, *[hop(w, 1) for w in own])

        def arrive(mask, slot, array):
            other = hop(array, 1)
            here[mask, slot] = [(array, (), ())]
            here[mask ^ 1, slot] = [(other, (), ())]
            return array

        def arrive_halves(mask, slot, low, high):
            for m, (a, b) in ((mask, (low, high)), (mask ^ 1, [hop(h, 1) for h in (low, high)])):
                here[m, slot] = [(a, (), (slice(None), pl.ds(0, half))), (b, (), (slice(None), pl.ds(half, half)))]

        tail = local - 1
        (head,) = pack(((0, 0, d_model),), *own)
        rest = pack(((1, 0, d_model),), *own)
        rest = list(rest) + list(pack(tuple((s, 0, d_model) for s in range(2, tail)) + ((tail, 0, half), (tail, half, half)), *own))
        packs = [head] + rest
        from_x, from_y = [], []
        for s in range(tail):
            from_x.append(arrive(2, s, hop(packs[s], 2)))
            from_y.append(arrive(4, s, hop(packs[s], 4)))
        x_low, x_high = [hop(h, 2) for h in packs[tail:]]
        y_low, y_high = [hop(h, 4) for h in packs[tail:]]
        arrive_halves(2, tail, x_low, x_high)
        arrive_halves(4, tail, y_low, y_high)
        for s in range(tail):
            arrive(6, s, hop(from_x[s], 4) if s < tail // 2 else hop(from_y[s], 2))
        arrive_halves(6, tail, hop(x_low, 4), hop(y_high, 2))

        stages = [
            [(m, s) for m in (0, 1) for s in range(local)],
            [(m, s) for s in (0, 1) for m in (2, 4, 3, 5)],
            [(m, s) for s in (2, 3) for m in (2, 4, 3, 5)],
            [(m, 4) for m in (2, 4, 3, 5)],
            [(m, s) for m in (6, 7) for s in (0, 2)],
            [(m, s) for m in (6, 7) for s in (1, 3)],
            [(6, 4), (7, 4)],
        ]
        flat = [entry for stage in stages for entry in stage]
        me = lax.axis_index("ep")
        masks = jnp.array([m for m, _ in flat], jnp.int32)
        slots = jnp.array([s for _, s in flat], jnp.int32)
        order = (me ^ masks) * local + slots
        address, gates, starts, counts = route_lists(tokens, routes, w_router)
        starts, counts = starts[order], counts[order]
        x_tiles = to_tiles(tokens.astype(jnp.float32))
        y, offset = None, 0
        for i, stage in enumerate(stages):
            y = run_stage(x_tiles, y, starts, counts, address, gates, offset, [here[e] for e in stage], (d_model, d_expert), i == len(stages) - 1)
            offset += len(stage)
        return y

    return jax.shard_map(device_step, mesh=mesh, in_specs=(row_spec, row_spec, P(None, None), expert_spec, expert_spec, expert_spec), out_specs=row_spec, check_vma=False)
```

```python
import functools

import jax
import jax.numpy as jnp
from jax import lax
from jax.experimental import pallas as pl
from jax.experimental.pallas import tpu as pltpu
from jax.sharding import PartitionSpec as P


LANES = 128
SUBLANES = 8
TILE = 256
GROUP = 16
BATCH = 8
PIECE = 4
ALIGN = 1024
LIST = 2048
PARTS = 16
AHEAD = 6
COST_FLOPS = 4_000_000_000


def route_lists(tokens, routes, w_router):
    num_tokens, _ = routes.shape
    num_experts = w_router.shape[1]
    chunks = tokens.shape[1] // LANES
    logits = jnp.dot(tokens, w_router, preferred_element_type=jnp.float32).T
    slots = routes.T
    experts = jnp.arange(num_experts, dtype=jnp.int32)
    hit = slots[:, None, :] == experts[None, :, None]
    picked = jnp.sum(jnp.where(hit, logits[None], 0.0), axis=1)
    gates = jax.nn.softmax(picked, axis=0)
    counts = jnp.sum(hit, axis=(0, 2), dtype=jnp.int32)
    starts = jnp.cumsum(counts) - counts
    keys = slots * num_tokens + jnp.arange(num_tokens, dtype=jnp.int32)[None, :]
    keys, gates = lax.sort((keys.reshape(-1), gates.reshape(-1)), num_keys=1, is_stable=False)
    token_at = keys % num_tokens
    address = token_at * chunks
    return jnp.pad(address, (0, LIST)), jnp.pad(gates, (0, LIST)), starts, counts


def pack_kernel(cuts, w_one, w_three, w_two, *refs):
    outs, (buffer, in_sem, out_sem) = refs[:len(cuts)], refs[len(cuts):]
    slots = sorted({s for s, _, _ in cuts})
    d_expert = w_one.shape[2]

    def loads(i, s):
        pairs = [(w_one.at[s], buffer.at[i, 0]), (w_three.at[s], buffer.at[i, 1])]
        for c in range(w_two.shape[2] // d_expert):
            pairs.append((w_two.at[s, :, pl.ds(c * d_expert, d_expert)], buffer.at[i, 2, pl.ds(c * d_expert, d_expert)]))
        return [pltpu.make_async_copy(a, b, in_sem.at[i, j]) for j, (a, b) in enumerate(pairs)]

    stores = [
        pltpu.make_async_copy(buffer.at[slots.index(s), :, pl.ds(row, size)], outs[k], out_sem.at[k])
        for k, (s, row, size) in enumerate(cuts)
    ]
    for i, s in enumerate(slots):
        for copy in loads(i, s):
            copy.start()
    for i, s in enumerate(slots):
        for copy in loads(i, s):
            copy.wait()
        for k, cut in enumerate(cuts):
            if cut[0] == s:
                stores[k].start()
    for copy in stores:
        copy.wait()


def pack(cuts, w_one, w_three, w_two):
    _, d_model, d_expert = w_one.shape
    num_slots = len({s for s, _, _ in cuts})
    return pl.pallas_call(
        functools.partial(pack_kernel, cuts),
        out_shape=[jax.ShapeDtypeStruct((3, size, d_expert), w_one.dtype) for _, _, size in cuts],
        in_specs=[pl.BlockSpec(memory_space=pl.ANY)] * 3,
        out_specs=[pl.BlockSpec(memory_space=pl.ANY)] * len(cuts),
        scratch_shapes=[
            pltpu.VMEM((num_slots, 3, d_model, d_expert), w_one.dtype),
            pltpu.SemaphoreType.DMA((num_slots, 2 + d_model // d_expert)),
            pltpu.SemaphoreType.DMA((len(cuts),)),
        ],
    )(w_one, w_three, w_two)


def next_tile(counts, e, t):
    more = (t + 1) * TILE < counts[e]
    return jnp.where(more, e, e + 1), jnp.where(more, t + 1, 0)


def part_reach(count, t, margin, entry, part_rows, num_parts):
    full = count - t * TILE >= TILE + margin
    return jnp.where(full, entry // part_rows + 1 - margin, num_parts)


def wait_parts(ready, which, copy, need, num_parts):
    have = ready[which]

    def one(k, _):
        copy(k).wait()

        @pl.when(k + AHEAD < num_parts)
        def _():
            copy(k + AHEAD).start()

        return 0

    lax.fori_loop(have, need, one, 0)
    ready[which] = jnp.maximum(have, need)


def row_pieces(base, chunks):
    return [pl.ds(pl.multiple_of(base + q * PIECE, PIECE), PIECE) for q in range(chunks // PIECE)]


def gather_kernel(num_experts, starts, counts, address, x_hbm, out, x_v, rows_v, tile_v, ready, x_sem, out_sem):
    chunks = tile_v.shape[2] // LANES
    num_parts = x_sem.shape[0]
    part_rows = x_v.shape[0] // num_parts

    def x_copy(k):
        rows = pl.ds(pl.multiple_of(k * part_rows, part_rows), part_rows)
        return pltpu.make_async_copy(x_hbm.at[rows], x_v.at[rows], x_sem.at[k])

    def out_copy(g):
        slot = lax.rem(g, 2)
        return pltpu.make_async_copy(tile_v.at[slot], out.at[g], out_sem.at[slot])

    def start_x(k, _):
        x_copy(k).start()
        return 0

    lax.fori_loop(0, AHEAD, start_x, 0)
    ready[0] = 0

    def tile(carry):
        e, t, g = carry
        at = starts[e] + t * TILE
        wait_parts(ready, 0, x_copy, part_reach(counts[e], t, 0, address[at + TILE - 1], part_rows, num_parts), num_parts)

        def gather_rows(i, _):
            for u in range(GROUP):
                target = i * (GROUP * chunks) + (u // SUBLANES) * (SUBLANES * chunks) + u % SUBLANES
                for q, piece in enumerate(row_pieces(address[at + i * GROUP + u], chunks)):
                    rows_v[pl.ds(target + q * (PIECE * SUBLANES), PIECE, stride=SUBLANES), :] = x_v[piece, :]
            return 0

        lax.fori_loop(0, TILE // GROUP, gather_rows, 0)

        @pl.when(g >= 2)
        def _():
            out_copy(g - 2).wait()

        tiled = rows_v[...].reshape(TILE // SUBLANES, chunks, SUBLANES, LANES)
        tile_v[lax.rem(g, 2)] = jnp.concatenate([tiled[:, c].reshape(TILE, LANES).astype(jnp.bfloat16) for c in range(chunks)], axis=1)
        out_copy(g).start()
        return next_tile(counts, e, t) + (g + 1,)

    g = lax.while_loop(lambda carry: carry[0] < num_experts, tile, (jnp.int32(0),) * 3)[2]
    wait_parts(ready, 0, x_copy, num_parts, num_parts)
    out_copy(g - 2).wait()
    out_copy(g - 1).wait()


def gather_tiles(x_rows, starts, counts, address, num_experts, d_model):
    chunks = d_model // LANES
    num_pairs = address.shape[0] - LIST
    smem = pl.BlockSpec(memory_space=pltpu.SMEM)
    hbm = pl.BlockSpec(memory_space=pl.ANY)
    return pl.pallas_call(
        functools.partial(gather_kernel, num_experts),
        out_shape=jax.ShapeDtypeStruct((num_pairs // TILE + num_experts, TILE, d_model), jnp.bfloat16),
        in_specs=[smem] * 3 + [hbm],
        out_specs=hbm,
        scratch_shapes=[
            pltpu.VMEM(x_rows.shape, jnp.float32),
            pltpu.VMEM((TILE * chunks, LANES), jnp.float32),
            pltpu.VMEM((2, TILE, d_model), jnp.bfloat16),
            pltpu.SMEM((1,), jnp.int32),
            pltpu.SemaphoreType.DMA((PARTS,)),
            pltpu.SemaphoreType.DMA((2,)),
        ],
        compiler_params=pltpu.CompilerParams(vmem_limit_bytes=64 * 2**20 - 2**16),
        cost_estimate=pl.CostEstimate(flops=10 * COST_FLOPS, bytes_accessed=num_pairs * d_model * 2, transcendentals=0),
        name="gather_tiles",
    )(starts, counts, address, x_rows)


def stage_kernel(first, last, offset, plan, d_model, d_expert, starts, counts, address, gates, tiles_hbm, *refs):
    refs = list(refs)
    y_hbm = None if first else refs.pop(0)
    num_arrays = 1 + max(piece[0] for pieces in plan for piece in pieces)
    weights, refs = refs[:num_arrays], refs[num_arrays:]
    out, y_v, w_v, tile_v, outs_v, cast_v, address_s, gates_s, ready, w_sem, tile_sem, list_sem, y_sem, out_sem = refs
    chunks = d_model // LANES
    stop = offset + len(plan)
    num_parts = y_sem.shape[0]
    part_rows = y_v.shape[0] // num_parts

    def part(ref, k):
        return ref.at[pl.ds(pl.multiple_of(k * part_rows, part_rows), part_rows)]

    def start_weights(e):
        slot = lax.rem(e, 2)
        for i, pieces in enumerate(plan):
            @pl.when(e == offset + i)
            def _(pieces=pieces):
                for array, source, target in pieces:
                    pltpu.make_async_copy(weights[array].at[source], w_v.at[(slot,) + target], w_sem.at[slot]).start()

    def wait_weights(e):
        slot = lax.rem(e, 2)
        pltpu.make_async_copy(w_v.at[slot], w_v.at[slot], w_sem.at[slot]).wait()

    def tile_copies(e, t, g):
        slot = lax.rem(g, 2)
        window = pl.multiple_of((starts[e] + t * TILE) // ALIGN * ALIGN, ALIGN)
        held = pl.ds(pl.multiple_of(slot * LIST, LIST), LIST)
        return [
            pltpu.make_async_copy(tiles_hbm.at[g], tile_v.at[slot], tile_sem.at[slot]),
            pltpu.make_async_copy(address.at[pl.ds(window, LIST)], address_s.at[held], list_sem.at[slot, 0]),
            pltpu.make_async_copy(gates.at[pl.ds(window, LIST)], gates_s.at[held], list_sem.at[slot, 1]),
        ]

    def y_copy(k):
        return pltpu.make_async_copy(part(y_hbm, k), part(y_v, k), y_sem.at[k])

    def count_tiles(e, total):
        return total + (counts[e] + TILE - 1) // TILE

    first_tile = lax.fori_loop(0, offset, count_tiles, jnp.int32(0))
    start_weights(jnp.int32(offset))
    for copy in tile_copies(jnp.int32(offset), jnp.int32(0), first_tile):
        copy.start()
    for i in range(2):
        ready[i] = 0
    if first:
        def clear(i, _):
            y_v[pl.ds(pl.multiple_of(i * 256, 256), 256), :] = jnp.zeros((256, LANES), jnp.float32)
            return 0

        lax.fori_loop(0, y_v.shape[0] // 256, clear, 0)
    else:
        def start_y(k, _):
            y_copy(k).start()
            return 0

        lax.fori_loop(0, AHEAD, start_y, 0)

    def add_rows(at, local, size):
        where = [row_pieces(address_s[at + u], chunks) for u in range(size)]
        sums = [[y_v[piece, :] for piece in pieces] for pieces in where]
        for u in range(size):
            gate = gates_s[at + u]
            terms = [outs_v[piece, :] * gate for piece in row_pieces(local + u * chunks, chunks)]
            sums[u] = [a + b for a, b in zip(sums[u], terms)]
        for u in range(size):
            for piece, value in zip(where[u], sums[u]):
                y_v[piece, :] = value

    if last:
        block = cast_v.shape[1]
        block_rows = block * chunks
        per_part = part_rows // block_rows

        def out_copy(i):
            slot = lax.rem(i, 2)
            return pltpu.make_async_copy(cast_v.at[slot], out.at[pl.ds(pl.multiple_of(i * block, block), block)], out_sem.at[slot])

        def store_part(k, _):
            for j in range(per_part):
                i = k * per_part + j

                @pl.when(i >= 2)
                def _():
                    out_copy(i - 2).wait()

                held = [y_v[pl.ds(i * block_rows + c, block, stride=chunks), :] for c in range(chunks)]
                cast_v[lax.rem(i, 2)] = jnp.concatenate([h.astype(jnp.bfloat16) for h in held], axis=1)
                out_copy(i).start()
            return 0
    else:
        def out_copy(k):
            return pltpu.make_async_copy(part(y_v, k), part(out, k), out_sem.at[k])

        def store_part(k, _):
            out_copy(k).start()
            return 0

    def tile(carry):
        e, t, g = carry
        slot = lax.rem(g, 2)
        w_slot = lax.rem(e, 2)
        begin = starts[e]
        count = counts[e]
        next_e, next_t = next_tile(counts, e, t)

        @pl.when(next_e < stop)
        def _():
            for copy in tile_copies(next_e, next_t, g + 1):
                copy.start()

        @pl.when(t == 0)
        def _():
            wait_weights(e)
            start_weights(e + 1)

        for copy in tile_copies(e, t, g):
            copy.wait()
        gate_pre = jnp.dot(tile_v[slot], w_v[w_slot, 0], preferred_element_type=jnp.float32)
        up_pre = jnp.dot(tile_v[slot], w_v[w_slot, 1], preferred_element_type=jnp.float32)
        hidden = (jax.nn.silu(gate_pre) * up_pre).astype(jnp.bfloat16)
        for c in range(d_model // d_expert):
            down = jnp.dot(hidden, w_v[w_slot, 2, c * d_expert:(c + 1) * d_expert], preferred_element_type=jnp.float32)
            down = down.astype(jnp.bfloat16).astype(jnp.float32)
            for k in range(d_expert // LANES):
                outs_v[pl.ds(c * (d_expert // LANES) + k, TILE, stride=chunks), :] = down[:, k * LANES:(k + 1) * LANES]

        here = slot * LIST + lax.rem(begin + t * TILE, ALIGN)
        final = address_s[here + TILE - 1]
        if not first:
            wait_parts(ready, 0, y_copy, part_reach(count, t, 0, final, part_rows, num_parts), num_parts)
        live = jnp.minimum(count - t * TILE, TILE)
        full = live // GROUP

        def add_group(i, _):
            for s in range(0, GROUP, BATCH):
                add_rows(here + i * GROUP + s, (i * GROUP + s) * chunks, BATCH)
            return 0

        def add_one(r, _):
            add_rows(here + r, r * chunks, 1)
            return 0

        lax.fori_loop(0, full, add_group, 0)
        lax.fori_loop(full * GROUP, live, add_one, 0)

        @pl.when(e == stop - 1)
        def _():
            settled = part_reach(count, t, 1, final, part_rows, num_parts)
            lax.fori_loop(ready[1], settled, store_part, 0)
            ready[1] = jnp.maximum(ready[1], settled)

        return next_e, next_t, g + 1

    lax.while_loop(lambda carry: carry[0] < stop, tile, (jnp.int32(offset), jnp.int32(0), first_tile))
    if last:
        num_blocks = (y_v.shape[0] // chunks) // block
        out_copy(num_blocks - 2).wait()
        out_copy(num_blocks - 1).wait()
    else:
        def drain(k, _):
            out_copy(k).wait()
            return 0

        lax.fori_loop(0, num_parts, drain, 0)


def run_stage(tiles, y_rows, num_rows, starts, counts, address, gates, offset, entries, shape, last):
    arrays, plan = [], []
    for entry in entries:
        pieces = []
        for array, source, target in entry:
            at = next((i for i, known in enumerate(arrays) if known is array), None)
            if at is None:
                at = len(arrays)
                arrays.append(array)
            pieces.append((at, source, target))
        plan.append(tuple(pieces))
    d_model, d_expert = shape
    chunks = d_model // LANES
    first = y_rows is None
    y_shape = (num_rows * chunks, LANES)
    smem = pl.BlockSpec(memory_space=pltpu.SMEM)
    hbm = pl.BlockSpec(memory_space=pl.ANY)
    operands = [address, gates, tiles] + ([] if first else [y_rows]) + arrays
    if last:
        out_shape = jax.ShapeDtypeStruct((num_rows, d_model), jnp.bfloat16)
    else:
        out_shape = jax.ShapeDtypeStruct(y_shape, jnp.float32)
    return pl.pallas_call(
        functools.partial(stage_kernel, first, last, offset, tuple(plan), d_model, d_expert),
        out_shape=out_shape,
        in_specs=[smem] * 2 + [hbm] * len(operands),
        out_specs=hbm,
        scratch_shapes=[
            pltpu.VMEM(y_shape, jnp.float32),
            pltpu.VMEM((2, 3, d_model, d_expert), jnp.bfloat16),
            pltpu.VMEM((2, TILE, d_model), jnp.bfloat16),
            pltpu.VMEM((TILE * chunks, LANES), jnp.float32),
            pltpu.VMEM((2, 128, d_model), jnp.bfloat16),
            pltpu.SMEM((2 * LIST,), jnp.int32),
            pltpu.SMEM((2 * LIST,), jnp.float32),
            pltpu.SMEM((2,), jnp.int32),
            pltpu.SemaphoreType.DMA((2,)),
            pltpu.SemaphoreType.DMA((2,)),
            pltpu.SemaphoreType.DMA((2, 2)),
            pltpu.SemaphoreType.DMA((PARTS,)),
            pltpu.SemaphoreType.DMA((PARTS,)),
        ],
        input_output_aliases={} if first or last else {5: 0},
        compiler_params=pltpu.CompilerParams(vmem_limit_bytes=64 * 2**20 - 2**16),
        cost_estimate=pl.CostEstimate(flops=len(plan) * COST_FLOPS, bytes_accessed=len(plan) * 6 * d_model * d_expert, transcendentals=0),
    )(starts, counts, *operands)


def solution(mesh):
    row_spec = P(("dp", "ep"), None)
    expert_spec = P("ep", None, None)
    size = mesh.shape["ep"]

    def hop(array, mask):
        return lax.ppermute(array, "ep", [(i, i ^ mask) for i in range(size)])

    def device_step(tokens, routes, w_router, *own):
        local, d_model, d_expert = own[0].shape
        half = d_model // 2
        blocks = d_model // d_expert
        here = {}

        def note(mask, w_one, w_three, w_two):
            for s in range(local):
                here[mask, s] = [(w_one, (s,), (0,)), (w_three, (s,), (1,))] + [
                    (w_two, (s, slice(None), pl.ds(c * d_expert, d_expert)), (2, pl.ds(c * d_expert, d_expert))) for c in range(blocks)
                ]

        note(0, *own)
        note(1, *[hop(w, 1) for w in own])

        def arrive(mask, slot, array):
            other = hop(array, 1)
            here[mask, slot] = [(array, (), ())]
            here[mask ^ 1, slot] = [(other, (), ())]
            return array

        def arrive_halves(mask, slot, low, high):
            for m, (a, b) in ((mask, (low, high)), (mask ^ 1, [hop(h, 1) for h in (low, high)])):
                here[m, slot] = [(a, (), (slice(None), pl.ds(0, half))), (b, (), (slice(None), pl.ds(half, half)))]

        tail = local - 1
        (head,) = pack(((0, 0, d_model),), *own)
        rest = pack(((1, 0, d_model),), *own)
        rest = list(rest) + list(pack(tuple((s, 0, d_model) for s in range(2, tail)) + ((tail, 0, half), (tail, half, half)), *own))
        packs = [head] + rest
        from_x, from_y = [], []
        for s in range(tail):
            from_x.append(arrive(2, s, hop(packs[s], 2)))
            from_y.append(arrive(4, s, hop(packs[s], 4)))
        x_low, x_high = [hop(h, 2) for h in packs[tail:]]
        y_low, y_high = [hop(h, 4) for h in packs[tail:]]
        arrive_halves(2, tail, x_low, x_high)
        arrive_halves(4, tail, y_low, y_high)
        for s in range(tail):
            arrive(6, s, hop(from_x[s], 4) if s < tail // 2 else hop(from_y[s], 2))
        arrive_halves(6, tail, hop(x_low, 4), hop(y_high, 2))

        stages = [
            [(m, s) for m in (0, 1) for s in range(local)],
            [(m, s) for s in (0, 1) for m in (2, 4, 3, 5)],
            [(m, s) for s in (2, 3) for m in (2, 4, 3, 5)],
            [(m, 4) for m in (2, 4, 3, 5)],
            [(m, s) for m in (6, 7) for s in (0, 2)],
            [(m, s) for m in (6, 7) for s in (1, 3)],
            [(6, 4), (7, 4)],
        ]
        flat = [entry for stage in stages for entry in stage]
        me = lax.axis_index("ep")
        masks = jnp.array([m for m, _ in flat], jnp.int32)
        slots = jnp.array([s for _, s in flat], jnp.int32)
        order = (me ^ masks) * local + slots
        address, gates, starts, counts = route_lists(tokens, routes, w_router)
        starts, counts = jnp.pad(starts[order], (0, 1)), jnp.pad(counts[order], (0, 1))
        x_rows = tokens.astype(jnp.float32).reshape(-1, LANES)
        tiles = gather_tiles(x_rows, starts, counts, address, len(flat), d_model)
        y, offset = None, 0
        for i, stage in enumerate(stages):
            y = run_stage(tiles, y, tokens.shape[0], starts, counts, address, gates, offset, [here[e] for e in stage], (d_model, d_expert), i == len(stages) - 1)
            offset += len(stage)
        return y

    return jax.shard_map(device_step, mesh=mesh, in_specs=(row_spec, row_spec, P(None, None), expert_spec, expert_spec, expert_spec), out_specs=row_spec, check_vma=False)
```

```python
import functools

import jax
import jax.numpy as jnp
from jax import lax
from jax.experimental import pallas as pl
from jax.experimental.pallas import tpu as pltpu
from jax.sharding import PartitionSpec as P


LANES = 128
SUBLANES = 8
TILE = 256
GROUP = 16
BATCH = 8
PIECE = 4
ALIGN = 1024
LIST = 2048
PARTS = 16
AHEAD = 6
CASTS = 8
SPLITS = (4, 2, 2, 2, 8)
COST_FLOPS = 4_000_000_000


def route_lists(tokens, routes, w_router):
    num_tokens, _ = routes.shape
    num_experts = w_router.shape[1]
    chunks = tokens.shape[1] // LANES
    logits = jnp.dot(tokens, w_router, preferred_element_type=jnp.float32).T
    slots = routes.T
    experts = jnp.arange(num_experts, dtype=jnp.int32)
    hit = slots[:, None, :] == experts[None, :, None]
    picked = jnp.sum(jnp.where(hit, logits[None], 0.0), axis=1)
    gates = jax.nn.softmax(picked, axis=0)
    counts = jnp.sum(hit, axis=(0, 2), dtype=jnp.int32)
    starts = jnp.cumsum(counts) - counts
    keys = slots * num_tokens + jnp.arange(num_tokens, dtype=jnp.int32)[None, :]
    keys, gates = lax.sort((keys.reshape(-1), gates.reshape(-1)), num_keys=1, is_stable=False)
    token_at = keys % num_tokens
    address = token_at * chunks
    return jnp.pad(address, (0, LIST)), jnp.pad(gates, (0, LIST)), starts, counts


def pack_kernel(cuts, w_one, w_three, w_two, *refs):
    count = len(cuts)
    outs, buffers, (in_sem, out_sem) = refs[:count], refs[count:2 * count], refs[2 * count:]
    d_expert = w_one.shape[2]

    def loads(k):
        s, row, size = cuts[k]
        pairs = [(w_one.at[s, pl.ds(row, size)], buffers[k].at[0]), (w_three.at[s, pl.ds(row, size)], buffers[k].at[1])]
        for c in range(w_two.shape[2] // d_expert):
            lo, hi = max(row, c * d_expert), min(row + size, (c + 1) * d_expert)
            if lo < hi:
                source = w_two.at[s, pl.ds(lo - c * d_expert, hi - lo), pl.ds(c * d_expert, d_expert)]
                pairs.append((source, buffers[k].at[2, pl.ds(lo - row, hi - lo)]))
        return [pltpu.make_async_copy(a, b, in_sem.at[k, j]) for j, (a, b) in enumerate(pairs)]

    stores = [pltpu.make_async_copy(buffers[k], outs[k], out_sem.at[k]) for k in range(count)]
    for k in range(count):
        for copy in loads(k):
            copy.start()
    for k in range(count):
        for copy in loads(k):
            copy.wait()
        stores[k].start()
    for copy in stores:
        copy.wait()


def pack(cuts, w_one, w_three, w_two):
    _, d_model, d_expert = w_one.shape
    return pl.pallas_call(
        functools.partial(pack_kernel, cuts),
        out_shape=[jax.ShapeDtypeStruct((3, size, d_expert), w_one.dtype) for _, _, size in cuts],
        in_specs=[pl.BlockSpec(memory_space=pl.ANY)] * 3,
        out_specs=[pl.BlockSpec(memory_space=pl.ANY)] * len(cuts),
        scratch_shapes=[pltpu.VMEM((3, size, d_expert), w_one.dtype) for _, _, size in cuts] + [
            pltpu.SemaphoreType.DMA((len(cuts), 2 + d_model // d_expert)),
            pltpu.SemaphoreType.DMA((len(cuts),)),
        ],
    )(w_one, w_three, w_two)


def next_tile(counts, e, t):
    more = (t + 1) * TILE < counts[e]
    return jnp.where(more, e, e + 1), jnp.where(more, t + 1, 0)


def part_reach(count, t, margin, entry, part_rows, num_parts):
    full = count - t * TILE >= TILE + margin
    return jnp.where(full, entry // part_rows + 1 - margin, num_parts)


def wait_parts(ready, which, copy, need, num_parts):
    have = ready[which]

    def one(k, _):
        copy(k).wait()

        @pl.when(k + AHEAD < num_parts)
        def _():
            copy(k + AHEAD).start()

        return 0

    lax.fori_loop(have, need, one, 0)
    ready[which] = jnp.maximum(have, need)


def row_pieces(base, chunks):
    return [pl.ds(pl.multiple_of(base + q * PIECE, PIECE), PIECE) for q in range(chunks // PIECE)]


def gather_kernel(num_experts, starts, counts, address, x_hbm, out, x_v, rows_v, tile_v, ready, x_sem, out_sem):
    chunks = tile_v.shape[2] // LANES
    num_parts = x_sem.shape[0]
    part_rows = x_v.shape[0] // num_parts

    def x_copy(k):
        rows = pl.ds(pl.multiple_of(k * part_rows, part_rows), part_rows)
        return pltpu.make_async_copy(x_hbm.at[rows], x_v.at[rows], x_sem.at[k])

    def out_copy(g):
        slot = lax.rem(g, 2)
        return pltpu.make_async_copy(tile_v.at[slot], out.at[g], out_sem.at[slot])

    def start_x(k, _):
        x_copy(k).start()
        return 0

    lax.fori_loop(0, AHEAD, start_x, 0)
    ready[0] = 0

    def tile(carry):
        e, t, g = carry
        at = starts[e] + t * TILE
        wait_parts(ready, 0, x_copy, part_reach(counts[e], t, 0, address[at + TILE - 1], part_rows, num_parts), num_parts)

        def gather_rows(i, _):
            for u in range(GROUP):
                target = i * (GROUP * chunks) + (u // SUBLANES) * (SUBLANES * chunks) + u % SUBLANES
                for q, piece in enumerate(row_pieces(address[at + i * GROUP + u], chunks)):
                    rows_v[pl.ds(target + q * (PIECE * SUBLANES), PIECE, stride=SUBLANES), :] = x_v[piece, :]
            return 0

        lax.fori_loop(0, TILE // GROUP, gather_rows, 0)

        @pl.when(g >= 2)
        def _():
            out_copy(g - 2).wait()

        tiled = rows_v[...].reshape(TILE // SUBLANES, chunks, SUBLANES, LANES)
        tile_v[lax.rem(g, 2)] = jnp.concatenate([tiled[:, c].reshape(TILE, LANES).astype(jnp.bfloat16) for c in range(chunks)], axis=1)
        out_copy(g).start()
        return next_tile(counts, e, t) + (g + 1,)

    g = lax.while_loop(lambda carry: carry[0] < num_experts, tile, (jnp.int32(0),) * 3)[2]
    wait_parts(ready, 0, x_copy, num_parts, num_parts)
    out_copy(g - 2).wait()
    out_copy(g - 1).wait()


def gather_tiles(x_rows, starts, counts, address, num_experts, d_model):
    chunks = d_model // LANES
    num_pairs = address.shape[0] - LIST
    smem = pl.BlockSpec(memory_space=pltpu.SMEM)
    hbm = pl.BlockSpec(memory_space=pl.ANY)
    return pl.pallas_call(
        functools.partial(gather_kernel, num_experts),
        out_shape=jax.ShapeDtypeStruct((num_pairs // TILE + num_experts, TILE, d_model), jnp.bfloat16),
        in_specs=[smem] * 3 + [hbm],
        out_specs=hbm,
        scratch_shapes=[
            pltpu.VMEM(x_rows.shape, jnp.float32),
            pltpu.VMEM((TILE * chunks, LANES), jnp.float32),
            pltpu.VMEM((2, TILE, d_model), jnp.bfloat16),
            pltpu.SMEM((1,), jnp.int32),
            pltpu.SemaphoreType.DMA((PARTS,)),
            pltpu.SemaphoreType.DMA((2,)),
        ],
        compiler_params=pltpu.CompilerParams(vmem_limit_bytes=64 * 2**20 - 2**16),
        cost_estimate=pl.CostEstimate(flops=10 * COST_FLOPS, bytes_accessed=num_pairs * d_model * 2, transcendentals=0),
        name="gather_tiles",
    )(starts, counts, address, x_rows)


def stage_kernel(first, last, offset, plan, d_model, d_expert, starts, counts, address, gates, tiles_hbm, *refs):
    refs = list(refs)
    y_hbm = None if first else refs.pop(0)
    num_arrays = 1 + max(piece[0] for pieces in plan for piece in pieces)
    weights, refs = refs[:num_arrays], refs[num_arrays:]
    out, y_v, w_v, tile_v, outs_v, cast_v, address_s, gates_s, ready, w_sem, tile_sem, list_sem, y_sem, out_sem = refs
    chunks = d_model // LANES
    stop = offset + len(plan)
    num_parts = y_sem.shape[0]
    part_rows = y_v.shape[0] // num_parts

    def part(ref, k):
        return ref.at[pl.ds(pl.multiple_of(k * part_rows, part_rows), part_rows)]

    def start_weights(e):
        slot = lax.rem(e, 2)
        for i, pieces in enumerate(plan):
            @pl.when(e == offset + i)
            def _(pieces=pieces):
                for array, source, target in pieces:
                    pltpu.make_async_copy(weights[array].at[source], w_v.at[(slot,) + target], w_sem.at[slot]).start()

    def wait_weights(e):
        slot = lax.rem(e, 2)
        pltpu.make_async_copy(w_v.at[slot], w_v.at[slot], w_sem.at[slot]).wait()

    def tile_copies(e, t, g):
        slot = lax.rem(g, 2)
        window = pl.multiple_of((starts[e] + t * TILE) // ALIGN * ALIGN, ALIGN)
        held = pl.ds(pl.multiple_of(slot * LIST, LIST), LIST)
        return [
            pltpu.make_async_copy(tiles_hbm.at[g], tile_v.at[slot], tile_sem.at[slot]),
            pltpu.make_async_copy(address.at[pl.ds(window, LIST)], address_s.at[held], list_sem.at[slot, 0]),
            pltpu.make_async_copy(gates.at[pl.ds(window, LIST)], gates_s.at[held], list_sem.at[slot, 1]),
        ]

    def y_copy(k):
        return pltpu.make_async_copy(part(y_hbm, k), part(y_v, k), y_sem.at[k])

    def count_tiles(e, total):
        return total + (counts[e] + TILE - 1) // TILE

    first_tile = lax.fori_loop(0, offset, count_tiles, jnp.int32(0))
    start_weights(jnp.int32(offset))
    for copy in tile_copies(jnp.int32(offset), jnp.int32(0), first_tile):
        copy.start()
    for i in range(2):
        ready[i] = 0
    if first:
        def clear(i, _):
            y_v[pl.ds(pl.multiple_of(i * 256, 256), 256), :] = jnp.zeros((256, LANES), jnp.float32)
            return 0

        lax.fori_loop(0, y_v.shape[0] // 256, clear, 0)
    else:
        def start_y(k, _):
            y_copy(k).start()
            return 0

        lax.fori_loop(0, AHEAD, start_y, 0)

    def add_rows(at, local, size):
        where = [row_pieces(address_s[at + u], chunks) for u in range(size)]
        sums = [[y_v[piece, :] for piece in pieces] for pieces in where]
        for u in range(size):
            gate = gates_s[at + u]
            terms = [outs_v[piece, :] * gate for piece in row_pieces(local + u * chunks, chunks)]
            sums[u] = [a + b for a, b in zip(sums[u], terms)]
        for u in range(size):
            for piece, value in zip(where[u], sums[u]):
                y_v[piece, :] = value

    if last:
        block = cast_v.shape[1]
        block_rows = block * chunks
        per_part = part_rows // block_rows

        def out_copy(i):
            slot = lax.rem(i, CASTS)
            return pltpu.make_async_copy(cast_v.at[slot], out.at[pl.ds(pl.multiple_of(i * block, block), block)], out_sem.at[slot])

        def store_part(k, _):
            for j in range(per_part):
                i = k * per_part + j

                @pl.when(i >= CASTS)
                def _():
                    out_copy(i - CASTS).wait()

                held = [y_v[pl.ds(i * block_rows + c, block, stride=chunks), :] for c in range(chunks)]
                cast_v[lax.rem(i, CASTS)] = jnp.concatenate([h.astype(jnp.bfloat16) for h in held], axis=1)
                out_copy(i).start()
            return 0
    else:
        def out_copy(k):
            return pltpu.make_async_copy(part(y_v, k), part(out, k), out_sem.at[k])

        def store_part(k, _):
            out_copy(k).start()
            return 0

    def tile(carry):
        e, t, g = carry
        slot = lax.rem(g, 2)
        w_slot = lax.rem(e, 2)
        begin = starts[e]
        count = counts[e]
        next_e, next_t = next_tile(counts, e, t)

        @pl.when(next_e < stop)
        def _():
            for copy in tile_copies(next_e, next_t, g + 1):
                copy.start()

        @pl.when(t == 0)
        def _():
            wait_weights(e)
            start_weights(e + 1)

        for copy in tile_copies(e, t, g):
            copy.wait()
        gate_pre = jnp.dot(tile_v[slot], w_v[w_slot, 0], preferred_element_type=jnp.float32)
        up_pre = jnp.dot(tile_v[slot], w_v[w_slot, 1], preferred_element_type=jnp.float32)
        hidden = (jax.nn.silu(gate_pre) * up_pre).astype(jnp.bfloat16)
        for c in range(d_model // d_expert):
            down = jnp.dot(hidden, w_v[w_slot, 2, c * d_expert:(c + 1) * d_expert], preferred_element_type=jnp.float32)
            down = down.astype(jnp.bfloat16).astype(jnp.float32)
            for k in range(d_expert // LANES):
                outs_v[pl.ds(c * (d_expert // LANES) + k, TILE, stride=chunks), :] = down[:, k * LANES:(k + 1) * LANES]

        here = slot * LIST + lax.rem(begin + t * TILE, ALIGN)
        final = address_s[here + TILE - 1]
        if not first:
            wait_parts(ready, 0, y_copy, part_reach(count, t, 0, final, part_rows, num_parts), num_parts)
        live = jnp.minimum(count - t * TILE, TILE)
        full = live // GROUP

        def add_group(i, _):
            for s in range(0, GROUP, BATCH):
                add_rows(here + i * GROUP + s, (i * GROUP + s) * chunks, BATCH)
            return 0

        def add_one(r, _):
            add_rows(here + r, r * chunks, 1)
            return 0

        lax.fori_loop(0, full, add_group, 0)
        lax.fori_loop(full * GROUP, live, add_one, 0)

        @pl.when(e == stop - 1)
        def _():
            settled = part_reach(count, t, 1, final, part_rows, num_parts)
            lax.fori_loop(ready[1], settled, store_part, 0)
            ready[1] = jnp.maximum(ready[1], settled)

        return next_e, next_t, g + 1

    lax.while_loop(lambda carry: carry[0] < stop, tile, (jnp.int32(offset), jnp.int32(0), first_tile))
    if last:
        num_blocks = (y_v.shape[0] // chunks) // block
        for i in range(CASTS):
            out_copy(num_blocks - CASTS + i).wait()
    else:
        def drain(k, _):
            out_copy(k).wait()
            return 0

        lax.fori_loop(0, num_parts, drain, 0)


def run_stage(tiles, y_rows, num_rows, starts, counts, address, gates, offset, entries, shape, last):
    arrays, plan = [], []
    for entry in entries:
        pieces = []
        for array, source, target in entry:
            at = next((i for i, known in enumerate(arrays) if known is array), None)
            if at is None:
                at = len(arrays)
                arrays.append(array)
            pieces.append((at, source, target))
        plan.append(tuple(pieces))
    d_model, d_expert = shape
    chunks = d_model // LANES
    first = y_rows is None
    y_shape = (num_rows * chunks, LANES)
    smem = pl.BlockSpec(memory_space=pltpu.SMEM)
    hbm = pl.BlockSpec(memory_space=pl.ANY)
    operands = [address, gates, tiles] + ([] if first else [y_rows]) + arrays
    if last:
        out_shape = jax.ShapeDtypeStruct((num_rows, d_model), jnp.bfloat16)
    else:
        out_shape = jax.ShapeDtypeStruct(y_shape, jnp.float32)
    return pl.pallas_call(
        functools.partial(stage_kernel, first, last, offset, tuple(plan), d_model, d_expert),
        out_shape=out_shape,
        in_specs=[smem] * 2 + [hbm] * len(operands),
        out_specs=hbm,
        scratch_shapes=[
            pltpu.VMEM(y_shape, jnp.float32),
            pltpu.VMEM((2, 3, d_model, d_expert), jnp.bfloat16),
            pltpu.VMEM((2, TILE, d_model), jnp.bfloat16),
            pltpu.VMEM((TILE * chunks, LANES), jnp.float32),
            pltpu.VMEM((CASTS, 128, d_model), jnp.bfloat16),
            pltpu.SMEM((2 * LIST,), jnp.int32),
            pltpu.SMEM((2 * LIST,), jnp.float32),
            pltpu.SMEM((2,), jnp.int32),
            pltpu.SemaphoreType.DMA((2,)),
            pltpu.SemaphoreType.DMA((2,)),
            pltpu.SemaphoreType.DMA((2, 2)),
            pltpu.SemaphoreType.DMA((PARTS,)),
            pltpu.SemaphoreType.DMA((PARTS,)),
        ],
        input_output_aliases={} if first or last else {5: 0},
        compiler_params=pltpu.CompilerParams(vmem_limit_bytes=64 * 2**20 - 2**16),
        cost_estimate=pl.CostEstimate(flops=len(plan) * COST_FLOPS, bytes_accessed=len(plan) * 6 * d_model * d_expert, transcendentals=0),
    )(starts, counts, *operands)


def solution(mesh):
    row_spec = P(("dp", "ep"), None)
    expert_spec = P("ep", None, None)
    size = mesh.shape["ep"]

    def hop(array, mask):
        return lax.ppermute(array, "ep", [(i, i ^ mask) for i in range(size)])

    def device_step(tokens, routes, w_router, *own):
        local, d_model, d_expert = own[0].shape
        blocks = d_model // d_expert
        here = {}

        def note(mask, w_one, w_three, w_two):
            for s in range(local):
                here[mask, s] = [(w_one, (s,), (0,)), (w_three, (s,), (1,))] + [
                    (w_two, (s, slice(None), pl.ds(c * d_expert, d_expert)), (2, pl.ds(c * d_expert, d_expert))) for c in range(blocks)
                ]

        note(0, *own)
        note(1, *[hop(w, 1) for w in own])

        segments = [[(i * d_model // n, d_model // n) for i in range(n)] for n in SPLITS]

        def arrive(mask, slot, arrays):
            for m in (mask, mask ^ 1):
                if m != mask:
                    arrays = [hop(a, 1) for a in arrays]
                here[m, slot] = [(a, (), (slice(None), pl.ds(row, size))) for a, (row, size) in zip(arrays, segments[slot])]

        cuts = [(s, row, size) for s in range(local) for row, size in segments[s]]
        packed = {}
        for group in (cuts[:1], cuts[1:4], cuts[4:]):
            packed.update(zip(group, pack(tuple(group), *own)))
        for s in range(local):
            mine = [packed[s, row, size] for row, size in segments[s]]
            from_x = [hop(a, 2) for a in mine]
            from_y = [hop(a, 4) for a in mine]
            arrive(2, s, from_x)
            arrive(4, s, from_y)
            split = len(mine) // 2
            arrive(6, s, [hop(from_x[k], 4) if k < split else hop(from_y[k], 2) for k in range(len(mine))])

        stages = [
            [(m, s) for m in (0, 1) for s in range(local)],
            [(m, s) for s in (0, 1) for m in (2, 4, 3, 5)],
            [(m, s) for s in (2, 3) for m in (2, 4, 3, 5)],
            [(m, 4) for m in (2, 4, 3, 5)],
        ] + [[(6, s), (7, s)] for s in range(local)]
        flat = [entry for stage in stages for entry in stage]
        me = lax.axis_index("ep")
        masks = jnp.array([m for m, _ in flat], jnp.int32)
        slots = jnp.array([s for _, s in flat], jnp.int32)
        order = (me ^ masks) * local + slots
        address, gates, starts, counts = route_lists(tokens, routes, w_router)
        starts, counts = jnp.pad(starts[order], (0, 1)), jnp.pad(counts[order], (0, 1))
        x_rows = tokens.astype(jnp.float32).reshape(-1, LANES)
        tiles = gather_tiles(x_rows, starts, counts, address, len(flat), d_model)
        y, offset = None, 0
        for i, stage in enumerate(stages):
            y = run_stage(tiles, y, tokens.shape[0], starts, counts, address, gates, offset, [here[e] for e in stage], (d_model, d_expert), i == len(stages) - 1)
            offset += len(stage)
        return y

    return jax.shard_map(device_step, mesh=mesh, in_specs=(row_spec, row_spec, P(None, None), expert_spec, expert_spec, expert_spec), out_specs=row_spec, check_vma=False)
```
